512 devices in a mesh: section: 16 (over x_hi, z), mp: 32 (over y, x_lo, core).
Axes of the slice: x: 4 (x_hi: 2, x_lo: 2; x = x_hi * 2 + x_lo), y: 8, z: 8, core: 2. Of those that a mesh axis runs over, the one named last changes fastest.
Arguments:
- embeddings: bfloat16 [16, 4, 128, 4096], P('section', None, None, 'mp'), may hold values from -6 to 6
- stored: bfloat16 [16, 15, 128, 4096], P('section', None, None, 'mp'), may hold values from -6 to 6
- dwa_weights: float32 [16, 16], replicated, may hold values from -2.4 to 2.4
- norm_gain: float32 [16, 4096], P('section'), may hold values from 0.5 to 1.5
- qkv_weight: bfloat16 [16, 4096, 3, 4096], P('section', None, None, 'mp')
- out_weight: bfloat16 [16, 4096, 4096], P('section', None, 'mp'), may hold values from -0.09375 to 0.09375
Outputs:
- layer_outputs: bfloat16 [16, 4, 128, 4096], P('section', None, None, 'mp')
The draws below stay inside these ranges and needn't reach their ends.
All inputs are finite; a program needn't handle non-finite values.
Results may differ from the reference program's by a relative error of at most 0.014.
Values may be sent and summed in bfloat16 or wider, within the bound.
No kernel may reach another device: no remote copies, remote signals or barrier semaphores. Data moves between devices by JAX's collectives and lax.ppermute only.
A program may use at most 64 MiB of HBM per device.

```python
import jax
import jax.numpy as jnp
from jax import lax

D = 4096
HEADS = 32
HEAD_DIM = 128
TOK = 128
TICKS = 4
SECTIONS = 16
SLOTS = 15


def draw_qkv_weight(key, part):
    base = jax.random.normal(key, (SECTIONS, D, 3, D), jnp.float32) * D ** (-0.5)
    return base.astype(jnp.bfloat16)


def block_levels(own_key, shape, split, low, largest):
    def one(axis_at, shards_of):
        draws = jax.random.uniform(jax.random.fold_in(jax.random.fold_in(own_key, 6), axis_at), (shards_of,), jnp.float32, low / len(split), largest / len(split))
        return jnp.repeat(jnp.exp(draws), shape[axis_at] // shards_of).reshape((-1,) + (1,) * (len(shape) - axis_at - 1))

    gain = one(*split[0])
    for cut in split[1:]:
        gain = gain * one(*cut)
    return gain


def scatter_about(own_key, dims, deviation, limit, cuts=(), held_as=jnp.bfloat16):
    result = deviation * jax.random.normal(own_key, dims, jnp.float32)
    if cuts:
        result = result * block_levels(own_key, dims, cuts, -0.22, 0.18)
    return jnp.clip(result, -limit, limit).astype(held_as)


def setup_inputs(seed: int = 0) -> dict:
    key_list = jax.random.split(jax.random.key(seed), 7)
    return {
        "embeddings": scatter_about(key_list[0], (SECTIONS, TICKS, TOK, D), 1.0, 6.0, ((0, 16), (3, 32))),
        "stored": scatter_about(key_list[1], (SECTIONS, SLOTS, TOK, D), 1.0, 6.0, ((0, 16), (3, 32))),
        "dwa_weights": scatter_about(key_list[2], (SECTIONS, SECTIONS), 0.4, 2.4, (), jnp.float32),
        "norm_gain": jnp.clip(1.0 + 0.1 * jax.random.normal(key_list[3], (SECTIONS, D), jnp.float32), 0.5, 1.5),
        "qkv_weight": draw_qkv_weight(jax.random.fold_in(key_list[6], 71), 0),
        "out_weight": scatter_about(key_list[5], (SECTIONS, D, D), D ** -0.5, 0.09375, ((0, 16), (2, 32))),
    }


EPS = 1e-06

def attend_heads(projected):
    length = projected.shape[0]
    query = projected[:, 0].astype(jnp.float32)
    key_rows = projected[:, 1].astype(jnp.float32)
    value_rows = projected[:, 2].astype(jnp.float32)
    scores = jnp.einsum('qhd,khd->hqk', query, key_rows) * projected.shape[3] ** (-0.5)
    causal = lax.broadcasted_iota(jnp.int32, (length, length), 0) >= lax.broadcasted_iota(jnp.int32, (length, length), 1)
    scores = jnp.where(causal[None], scores, -1e+30)
    row_max = lax.optimization_barrier(jnp.max(scores, axis=2, keepdims=True))
    weights = jnp.exp(scores - row_max)
    probs = (weights / lax.optimization_barrier(jnp.sum(weights, axis=2, keepdims=True))).astype(jnp.bfloat16)
    mixed = jnp.einsum('hqk,khd->qhd', probs.astype(jnp.float32), value_rows)
    return mixed.astype(jnp.bfloat16).reshape(length, -1)

def apply_layer(inputs, gain_row, weight_in, weight_out):
    length = inputs.shape[0]
    values = inputs.astype(jnp.float32)
    inverse = lax.rsqrt(lax.optimization_barrier(jnp.mean(values * values, axis=1, keepdims=True)) + EPS)
    normed = (values * inverse * gain_row).astype(jnp.bfloat16)
    projected = jnp.dot(normed, weight_in.reshape(D, 3 * D), preferred_element_type=jnp.float32).astype(jnp.bfloat16)
    projected = projected.reshape(length, 3, HEADS, HEAD_DIM)
    mixed = attend_heads(projected)
    attn = jnp.dot(mixed, weight_out, preferred_element_type=jnp.float32)
    return (values + attn).astype(jnp.bfloat16)

def reference(embeddings, stored, dwa_weights, norm_gain, qkv_weight, out_weight):
    triangle = jnp.tril(jnp.ones((SECTIONS, SECTIONS), jnp.float32))
    mixing = dwa_weights * triangle
    history = [jnp.concatenate([stored[s], jnp.zeros((TICKS, TOK, D), jnp.bfloat16)], axis=0) for s in range(SECTIONS)]
    results = [[None] * TICKS for s in range(SECTIONS)]
    for step_index in range(TICKS):
        fresh_rows = []
        for section_idx in range(SECTIONS):
            summed = mixing[section_idx, 0] * embeddings[section_idx, step_index].astype(jnp.float32)
            slot_index = step_index - section_idx + SECTIONS - 1
            for source in range(section_idx):
                summed = summed + mixing[section_idx, source + 1] * history[source][slot_index].astype(jnp.float32)
            inputs = summed.astype(jnp.bfloat16)
            fresh_rows.append(apply_layer(inputs, norm_gain[section_idx], qkv_weight[section_idx], out_weight[section_idx]))
        for section_idx in range(SECTIONS):
            slot_index = step_index - section_idx + SECTIONS - 1
            history[section_idx] = history[section_idx].at[slot_index].set(fresh_rows[section_idx])
            results[section_idx][step_index] = fresh_rows[section_idx]
    return jnp.stack([jnp.stack(row_list) for row_list in results])
```

```python
import jax
import jax.numpy as jnp
from jax import lax
from jax.sharding import Mesh, PartitionSpec as P

HEAD_DIM = 128
EPS = 1e-06
CORE_SWAP = ((0, 1), (1, 0))

SECTION = ("xh", "z")
CHIPS = ("y", "xl")


def spread(piece, axis):
    count = lax.axis_size(axis)
    return lax.all_to_all(jnp.broadcast_to(piece[None], (count, *piece.shape)), axis, 0, 0, tiled=True)


def in_core_order(core, own, other):
    return jnp.where(core == 0, jnp.stack([own, other]), jnp.stack([other, own]))


def attend(core, projected, partner_projected):
    tokens = projected.shape[0]
    pair = jnp.stack([projected, partner_projected])
    pair = pair.reshape(2, tokens, 3, HEAD_DIM)
    both = lax.all_gather(pair[:, :, 1:], "c")
    other = lax.dynamic_index_in_dim(both, 1 - core, 0, keepdims=False)[::-1]
    query = pair[:, :, 0]
    scale = HEAD_DIM ** (-0.5)
    dims = (((2,), (2,)), ((0,), (0,)))
    near = lax.dot_general(query, pair[:, :, 1], dims, preferred_element_type=jnp.float32) * scale
    far = lax.dot_general(query, other[:, :, 0], dims, preferred_element_type=jnp.float32) * scale
    row = lax.broadcasted_iota(jnp.int32, (tokens, tokens), 0)
    col = lax.broadcasted_iota(jnp.int32, (tokens, tokens), 1)
    near = jnp.where((row >= col)[None], near, -1e30)
    far = jnp.where(core == 1, far, -1e30)
    top = jnp.maximum(jnp.max(near, axis=2, keepdims=True), jnp.max(far, axis=2, keepdims=True))
    near = jnp.exp(near - top)
    far = jnp.exp(far - top)
    total = jnp.sum(near, axis=2, keepdims=True) + jnp.sum(far, axis=2, keepdims=True)
    near = (near / total).astype(jnp.bfloat16)
    far = (far / total).astype(jnp.bfloat16)
    dims = (((2,), (1,)), ((0,), (0,)))
    mixed = lax.dot_general(near, pair[:, :, 2], dims, preferred_element_type=jnp.float32)
    mixed = mixed + lax.dot_general(far, other[:, :, 1], dims, preferred_element_type=jnp.float32)
    mixed = mixed.astype(jnp.bfloat16)
    return in_core_order(core, mixed[0], mixed[1])


def local(embeddings, stored, dwa_weights, norm_gain, qkv_weight, out_weight):
    sections = lax.axis_size(SECTION)
    rank = lax.axis_index(SECTION)
    core = lax.axis_index("c")
    ticks, length, width = embeddings.shape[1:]
    half = length // 2
    features = norm_gain.shape[1]
    blocks = features // width
    forward = tuple((s, s + 1) for s in range(sections - 1))

    mixing = dwa_weights * jnp.tril(jnp.ones((sections, sections), jnp.float32))
    mixing = jnp.concatenate([mixing, jnp.zeros((ticks, sections), jnp.float32)], axis=0)
    rows = lax.dynamic_slice_in_dim(mixing, rank, ticks, axis=0)
    newest = lax.dynamic_index_in_dim(rows, rank, 1, keepdims=False)

    weight_in = qkv_weight[0].reshape(features, 3 * width)
    weight_out = out_weight[0]
    partner_in = lax.ppermute(weight_in, "c", CORE_SWAP)
    partner_out = lax.ppermute(weight_out, "c", CORE_SWAP)
    gain = norm_gain[0].reshape(blocks, 1, width)

    target = lax.broadcasted_iota(jnp.int32, (sections, 1, 1), 0)
    outgoing = jnp.concatenate([stored[0], embeddings[0, :1]], axis=0)[::-1]
    outgoing = jnp.where(target == rank, embeddings[0, :1], outgoing)
    incoming = lax.all_to_all(
        outgoing.reshape(sections * 2, half, width), SECTION + ("c",), 0, 0, tiled=True
    )
    incoming = incoming.reshape(sections, 2, half, width).astype(jnp.float32)
    source = lax.broadcasted_iota(jnp.int32, (1, sections), 1)
    shifted = jnp.concatenate([rows[:, 1:], jnp.zeros((ticks, 1), jnp.float32)], axis=1)
    weights = jnp.where(source < rank, shifted, 0.0)
    first = jnp.where(source[0] == rank, rows[0, 0], weights[0])
    summed = jnp.sum(first[:, None, None, None] * incoming, axis=0)
    later = [
        jnp.sum(weights[r][:, None, None, None] * incoming, axis=0) for r in range(1, ticks)
    ]

    embedded = lax.all_gather(embeddings[0, 1:].reshape(ticks - 1, 2, half, width), "c")
    embedded = lax.dynamic_index_in_dim(embedded, core, 2, keepdims=False)

    results = []
    for tick in range(ticks):
        if tick:
            summed = rows[0, 0] * embedded[:, tick - 1].astype(jnp.float32)
            summed = summed + carried[0] + newest[0] * fresh.astype(jnp.float32)
            later = [
                carried[r] + newest[r] * fresh.astype(jnp.float32) for r in range(1, ticks - tick)
            ]
        inputs = summed.astype(jnp.bfloat16)
        if later:
            carried = lax.ppermute(jnp.stack(later), SECTION, forward)
        values = spread(inputs, CHIPS).reshape(blocks, half, width).astype(jnp.float32)
        inverse = lax.rsqrt(jnp.mean(values * values, axis=(0, 2), keepdims=True) + EPS)
        normed = (values * inverse * gain).astype(jnp.bfloat16)
        normed = jnp.transpose(normed, (1, 0, 2)).reshape(half, features)
        projected = jnp.dot(normed, weight_in, preferred_element_type=jnp.float32)
        partner_projected = jnp.dot(normed, partner_in, preferred_element_type=jnp.float32)
        mixed = attend(core, projected.astype(jnp.bfloat16), partner_projected.astype(jnp.bfloat16))
        mixed = spread(mixed, CHIPS).reshape(blocks, half, width)
        mixed = jnp.transpose(mixed, (1, 0, 2)).reshape(half, features)
        attn = jnp.dot(mixed, weight_out, preferred_element_type=jnp.float32)
        partner_attn = jnp.dot(mixed, partner_out, preferred_element_type=jnp.float32)
        attn = in_core_order(core, attn, partner_attn)
        made = (inputs.astype(jnp.float32) + attn).astype(jnp.bfloat16)
        results.append(made)
        if tick + 1 < ticks:
            fresh = lax.ppermute(made, SECTION, forward)
    both = lax.all_gather(jnp.stack(results), "c")
    mine = lax.dynamic_index_in_dim(both, core, 2, keepdims=False)
    return jnp.transpose(mine, (1, 0, 2, 3)).reshape(1, ticks, length, width)


def solution(mesh):
    split = Mesh(mesh.devices.reshape(2, 8, 8, 2, 2), ("xh", "z", "y", "xl", "c"))
    mp = ("y", "xl", "c")
    in_specs = (
        P(SECTION, None, None, mp),
        P(SECTION, None, None, mp),
        P(),
        P(SECTION, None),
        P(SECTION, None, None, mp),
        P(SECTION, None, mp),
    )
    out_specs = P(SECTION, None, None, mp)
    return jax.shard_map(local, mesh=split, in_specs=in_specs, out_specs=out_specs, check_vma=False)
```
